32 devices in a mesh: dp: 2 (over z, core), sp: 16 (over x, y).
Axes of the slice: x: 4, y: 4, z: 1, core: 2. Of those that a mesh axis runs over, the one named last changes fastest.
The devices are a block of a 4x4x8 slice.
Arguments:
- x: bfloat16 [16384, 2560], P(('dp', 'sp')), parts along dimension 0
- gain: bfloat16 [2560], replicated
- wq: bfloat16 [2560, 2048], P('sp')
- wk: bfloat16 [2560, 1024], P('sp')
- wv: bfloat16 [2560, 1024], P('sp')
- wo: bfloat16 [2048, 2560], P('sp')
Outputs:
- output: bfloat16 [16384, 2560], P(('dp', 'sp')), parts along dimension 0
There are 2 independent parts. The reference program is written for one: setup_inputs(seed, part) draws one part's arguments, and reference() takes and returns one part's arrays. A program takes and returns all parts, laid end to end along the dimension named above; an argument that names none is the same for every part.
All inputs are finite; a program needn't handle non-finite values.
Results may differ from the reference program's by a relative error of at most 0.012.
Values are sent between devices in bfloat16 or wider.
A program may use at most 768 MiB of HBM per device.

```python
import jax
import jax.numpy as jnp
from jax import lax

ROWS = 8192
D = 2560
HEADS = 8
KV_HEADS = 4
HEAD = 256
THETA = 10000


def setup_inputs(seed: int = 0, part: int = 0) -> dict:
    kx, kn, kq, kk, kv, ko = jax.random.split(jax.random.key(seed), 6)

    def weights(key, rows, columns):
        return jax.random.normal(key, (rows, columns), jnp.float32) * rows**-0.5

    drawn = {
        "x": jax.random.normal(jax.random.fold_in(kx, part), (ROWS, D), jnp.float32),
        "gain": 1 + 0.1 * jax.random.normal(kn, (D,), jnp.float32),
        "wq": 2 * weights(kq, D, HEADS * HEAD),
        "wk": 2 * weights(kk, D, KV_HEADS * HEAD),
        "wv": 4 * weights(kv, D, KV_HEADS * HEAD),
        "wo": weights(ko, HEADS * HEAD, D),
    }
    return {k: v.astype(jnp.bfloat16) for k, v in drawn.items()}


def normed(x, gain):
    wide = x.astype(jnp.float32)
    scale = lax.rsqrt(jnp.mean(wide * wide, -1, keepdims=True) + 1e-6)
    return (wide * scale * gain.astype(jnp.float32)).astype(jnp.bfloat16)


def turned(t, place, theta):
    half = t.shape[-1] // 2
    angle = place.astype(jnp.float32)[:, None] * theta ** (-jnp.arange(half, dtype=jnp.float32) / half)
    cos, sin = jnp.cos(angle)[:, None], jnp.sin(angle)[:, None]
    a, b = t[..., :half].astype(jnp.float32), t[..., half:].astype(jnp.float32)
    return jnp.concatenate([a * cos - b * sin, b * cos + a * sin], -1).astype(jnp.bfloat16)


def matmul(a, w):
    return jnp.dot(a, w, preferred_element_type=jnp.float32).astype(jnp.bfloat16)


def einsum(form, a, b):
    return jnp.einsum(form, a.astype(jnp.float32), b.astype(jnp.float32))


def attention(q, k, v):
    scores = einsum("tgsd,ugd->gstu", q, k) * q.shape[-1] ** -0.5
    token = jnp.arange(q.shape[0])
    scores = jnp.where(token[:, None] >= token, scores, -jnp.inf)
    weights = jax.nn.softmax(scores, -1).astype(jnp.bfloat16)
    return einsum("gstu,ugd->tgsd", weights, v).astype(jnp.bfloat16)


def reference(x, gain, wq, wk, wv, wo):
    a, place = normed(x, gain), jnp.arange(ROWS)
    q = turned(matmul(a, wq).reshape(ROWS, HEADS, HEAD), place, THETA).reshape(ROWS, KV_HEADS, -1, HEAD)
    k = turned(matmul(a, wk).reshape(ROWS, KV_HEADS, HEAD), place, THETA)
    v = matmul(a, wv).reshape(ROWS, KV_HEADS, HEAD)
    seen = attention(q, k, v).reshape(ROWS, HEADS * HEAD)
    return (x.astype(jnp.float32) + jnp.dot(seen, wo, preferred_element_type=jnp.float32)).astype(jnp.bfloat16)
```

```python
import functools

import jax
import jax.numpy as jnp
from jax import lax
from jax.experimental import pallas as pl
from jax.experimental.pallas import tpu as pltpu

NEG = -1e30
HIDDEN = 2 * NEG
LOG2E = 1.4426950408889634
VMEM = 60 * 2**20


def _dot(a, b, ca, cb):
    return lax.dot_general(a, b, (((ca,), (cb,)), ((), ())), preferred_element_type=jnp.float32)


import math

from jax.sharding import PartitionSpec as P

HEAD = 256
THETA = 10000
MESH = pl.DeviceIdType.MESH


def normed(x, gain):
    wide = x.astype(jnp.float32)
    scale = lax.rsqrt(jnp.mean(wide * wide, -1, keepdims=True) + 1e-6)
    return (wide * scale * gain.astype(jnp.float32)).astype(jnp.bfloat16)


class Place:
    def __init__(self, side):
        self.side = side
        self.c = lax.rem(lax.axis_index("dp"), 2)
        self.me = lax.axis_index("sp")
        hi, lo = lax.div(self.me, side), lax.rem(self.me, side)
        self.r = (1 - self.c) * hi + self.c * lo
        self.p = (1 - self.c) * lo + self.c * hi

    def at(self, dr, dp):
        r, p = lax.rem(self.r + dr + self.side, self.side), lax.rem(self.p + dp + self.side, self.side)
        return self.block(r, p), r, p

    def block(self, r, p):
        return (1 - self.c) * (r * self.side + p) + self.c * (p * self.side + r)


def _remote(src, dst, send, recv, index, axis="sp"):
    return pltpu.make_async_remote_copy(src_ref=src, dst_ref=dst, send_sem=send, recv_sem=recv, device_id={axis: index}, device_id_type=MESH)


def _greet(place, others):
    barrier = pltpu.get_barrier_semaphore()
    for other in others:
        pl.semaphore_signal(barrier, inc=1, device_id=other, device_id_type=MESH)
    pl.semaphore_wait(barrier, len(others))


def _project(side, a, freq, wq, wk, wv, q_out, k_out, v_out, abuf, wbuf, cos_s, sin_s, asem, lsem, w1s, w1r, w2s, w2r, xs, xr):
    place = Place(side)
    own, share = a.shape[0], wq.shape[0]
    half = own // 2
    parts, off = [], 0
    for w in (wq, wk, wv):
        width = w.shape[1] // side
        parts.append((w, width, off))
        off += width
    rows = lambda index: pl.ds(pl.multiple_of(index * share, 32), share)
    mine = rows(place.me)
    _greet(place, [{"sp": place.at(*d)[0]} for d in ((0, 1), (0, 2), (0, 3), (1, 0), (-1, 0))])

    w1 = {}
    for d in range(1, side):
        index, _, to = place.at(0, d)
        for i, (w, width, at) in enumerate(parts):
            columns = pl.ds(pl.multiple_of(to * width, 128), width)
            w1[d, i] = _remote(w.at[:, columns], wbuf.at[mine, pl.ds(at, width)], w1s.at[d, i], w1r.at[d, i], index)
            w1[d, i].start()
    for i, (w, width, at) in enumerate(parts):
        columns = pl.ds(pl.multiple_of(place.p * width, 128), width)
        w1[0, i] = pltpu.make_async_copy(w.at[:, columns], wbuf.at[mine, pl.ds(at, width)], lsem.at[i])
        w1[0, i].start()
    right, left = place.at(0, 1)[0], place.at(0, -1)[0]
    part = lambda h: pl.ds(h * half, half)
    x = {}
    for s, to, order in ((0, right, (0, 1)), (1, left, (1, 0))):
        for h in order:
            x[s, h] = _remote(a.at[part(h), :], abuf.at[s + 1, part(h), :], xs.at[s, h], xr.at[s, h], to)
            x[s, h].start()
    a_own = pltpu.make_async_copy(a, abuf.at[0], asem)
    a_own.start()

    down, up = place.at(1, 0)[0], place.at(-1, 0)[0]
    w2 = {}
    for d in range(side):
        for i in range(3):
            if d:
                w1[d, i].wait_recv()
            else:
                w1[d, i].wait()
        block = wbuf.at[rows(place.at(0, -d)[0]), :]
        for s, to in ((0, down), (1, up)):
            w2[s, d] = _remote(block, block, w2s.at[s, d], w2r.at[s, d], to)
            w2[s, d].start()

    def table(n, _):
        slot, h = lax.div(n, 2), lax.rem(n, 2)
        q = lax.rem(place.p + side + lax.rem(slot + 1, 2) * lax.div(slot, 2) - lax.rem(slot, 2) * (1 - 3 * lax.div(slot, 2)), side)
        first = place.block(place.r, q) * own + h * half
        angle = (lax.broadcasted_iota(jnp.int32, (half, HEAD // 2), 0) + first).astype(jnp.float32) * freq[...]
        cos_s[n] = jnp.cos(angle)
        sin_s[n] = jnp.sin(angle)
        return 0

    lax.fori_loop(0, 2 * side, table, 0)

    def pass_x(s, h, to):
        x[s, h].wait_recv()
        x[2, h] = _remote(abuf.at[s + 1, part(h), :], abuf.at[3, part(h), :], xs.at[2, h], xr.at[2, h], to)
        x[2, h].start()

    for d in range(side):
        for s, to, dr in ((0, down, -1), (1, up, 1)):
            w2[s, d].wait_recv()
            if (d < side // 2) == (s == 0):
                block = wbuf.at[rows(place.at(dr, -d)[0]), :]
                w2[2, d] = _remote(block, block, w2s.at[2, d], w2r.at[2, d], to)
                w2[2, d].start()
        if d == 1:
            pass_x(0, 0, right)
            pass_x(1, 1, left)
    for d in range(side):
        w2[2, d].wait_recv()
    a_own.wait()

    def turn(t, cos, sin):
        t = t.astype(jnp.bfloat16)
        lo, hi = t[:, : HEAD // 2].astype(jnp.float32), t[:, HEAD // 2 :].astype(jnp.float32)
        return jnp.concatenate([lo * cos - hi * sin, hi * cos + lo * sin], 1).astype(jnp.bfloat16)

    def project(n, _):
        for when, (s, h) in ((3, (0, 1)), (4, (1, 0)), (6, (2, 0)), (7, (2, 1))):
            pl.when(n == when)(x[s, h].wait_recv)
        slot, h = lax.div(n, 2), lax.rem(n, 2)
        q = lax.rem(place.p + side + lax.rem(slot + 1, 2) * lax.div(slot, 2) - lax.rem(slot, 2) * (1 - 3 * lax.div(slot, 2)), side)
        here = pl.ds(pl.multiple_of(h * half, half), half)
        got = _dot(abuf[slot, here, :], wbuf[...], 1, 0)
        cos, sin = cos_s[n], sin_s[n]
        g = parts[0][1] // HEAD
        for j in range(g):
            q_out[q * g + j, here, :] = turn(got[:, j * HEAD : (j + 1) * HEAD], cos, sin)
        k_out[q, here, :] = turn(got[:, g * HEAD : (g + 1) * HEAD], cos, sin)
        v_out[q, :, here] = got[:, (g + 1) * HEAD :].astype(jnp.bfloat16).T
        return 0

    lax.fori_loop(0, 2 * side, project, 0)

    for copies in (w1, w2, x):
        for key, copy in copies.items():
            if not (copies is w1 and key[0] == 0):
                copy.wait_send()


def _attention(side, scale, q, k, v, wo, o_out, wo_out, kbuf, vbuf, obuf, top_s, mix_s, lsem, ks, kr, osend, orecv, olocal, g1s, g1r, g2s, g2r, ds, dr, glocal):
    place = Place(side)
    g = q.shape[0] // side
    own, d = q.shape[1], q.shape[2]
    low = q.dtype
    e = scale * LOG2E
    down, up = place.at(1, 0)[0], place.at(-1, 0)[0]
    right, left = place.at(0, 1)[0], place.at(0, -1)[0]
    partner = lax.axis_index("dp") + 1 - 2 * place.c
    _greet(place, [{"sp": place.at(*t)[0]} for t in ((0, 1), (0, 2), (0, 3), (1, 0), (2, 0), (3, 0))] + [{"dp": partner}])

    share, wide = wo.shape[0], wo.shape[1] // 2
    half = pl.ds(pl.multiple_of(place.c * wide, 128), wide)

    def piece(to_r, to_p):
        return wo_out.at[pl.ds(pl.multiple_of(place.at(to_r, to_p)[0] * share, share), share), half]

    g1 = {t: _remote(wo.at[:, half], piece(0, 0), g1s.at[t], g1r.at[t], place.at(t, 0)[0]) for t in (1, 3, 2)}
    for copy in g1.values():
        copy.start()
    whole = pltpu.make_async_copy(wo, wo_out.at[pl.ds(pl.multiple_of(place.me * share, share), share), :], glocal)
    whole.start()

    def along(s, t):
        if s == 2:
            block, to = piece(-t, -1 if t < side // 2 else 1), right if t < side // 2 else left
        else:
            block, to = piece(-t, 0), (right, left)[s]
        if t == 0 and s < 2:
            return _remote(wo.at[:, half], block, g2s.at[s, t], g2r.at[s, t], to)
        return _remote(block, block, g2s.at[s, t], g2r.at[s, t], to)

    def across(n, t, to_p):
        block = piece(-t, to_p)
        return _remote(block, block, ds.at[n, t], dr.at[n, t], partner, "dp")

    def wo_start():
        for t in range(side):
            if t:
                g1[t].wait_recv()
                across(0, t, 0).start()
            for s in range(2):
                along(s, t).start()

    def wo_next(t):
        for s in range(2):
            along(s, t).wait_recv()
            across(s + 1, t, (-1, 1)[s]).start()
            if (t < side // 2) == (s == 0):
                along(2, t).start()

    def wo_last(t):
        along(2, t).wait_recv()
        across(3, t, 2).start()

    def wo_end():
        for n, to_p in enumerate((0, -1, 1, 2)):
            for t in range(side):
                if n or t:
                    across(n, t, to_p).wait()
        for t in range(side):
            for s in range(3):
                along(s, t).wait_send()
            if t:
                g1[t].wait_send()
        whole.wait()

    def kv(s, b, to):
        slot, src = (s + 1, (k, v)) if s < 2 else (3, (kbuf.at[s - 1], vbuf.at[s - 1]))
        i = min(s, 2)
        return [_remote(f.at[b], t.at[slot, b], ks.at[i, b, n], kr.at[i, b, n], to) for n, (f, t) in enumerate(zip(src, (kbuf, vbuf)))]

    for n in range(side):
        for s, to, b in ((0, down, n), (1, up, (n + side // 2) % side)):
            for copy in kv(s, b, to):
                copy.start()
    mine = [pltpu.make_async_copy(f, t.at[0], lsem.at[n]) for n, (f, t) in enumerate(((k, kbuf), (v, vbuf)))]
    for copy in mine:
        copy.start()
    top_s[...] = jnp.full(top_s.shape, NEG, jnp.float32)
    mix_s[...] = jnp.zeros(mix_s.shape, jnp.float32)
    ones = jnp.ones((8, own), low)
    for copy in mine:
        copy.wait()

    def unit(a, s, b, masked=False):
        keys = kbuf[s, b]
        scores = [_dot(keys, q[a * g + j], 1, 1) for j in range(g)]
        weights, keeps = [], []
        for j, t in enumerate(scores):
            if masked:
                seen = lax.broadcasted_iota(jnp.int32, (own, own), 1) >= lax.broadcasted_iota(jnp.int32, (own, own), 0)
                t = jnp.where(seen, t, HIDDEN)
            old = top_s[a * g + j]
            top = jnp.maximum(old, t.max(axis=0, keepdims=True))
            top_s[a * g + j] = top
            weights.append(jnp.exp2((t - top) * e).astype(low))
            keeps.append(jnp.exp2((old - top) * e))
        values = jnp.concatenate([vbuf[s, b], ones], axis=0)
        for j, (w, keep) in enumerate(zip(weights, keeps)):
            mix_s[a * g + j] = mix_s[a * g + j] * keep + _dot(values, w, 1, 0)

    def own_keys(b, _):
        unit(b, 0, b, True)
        lax.fori_loop(b + 1, side, lambda a, _: (unit(a, 0, b), 0)[1], 0)
        return 0

    lax.fori_loop(0, side, own_keys, 0)
    wo_start()

    def before(dr):
        there = lax.rem(place.r + dr + side, side)
        return lax.div(place.r - there + side - 1, side)

    def first_seeing(dr, b):
        return (1 - place.c) * (1 - before(dr)) * side + place.c * (b + 1 - before(dr))

    def neighbours(n, _):
        for s, dr, b, to in ((0, -1, n, down), (1, 1, lax.rem(n + side // 2, side), up)):
            for copy in kv(s, b, to):
                copy.wait_recv()

            @pl.when(n < side // 2)
            def _():
                for copy in kv(s + 2, b, to):
                    copy.start()

            lax.fori_loop(first_seeing(dr, b), side, lambda a, _: (unit(a, s + 1, b), 0)[1], 0)
        for t in range(side):
            pl.when(n == t)(functools.partial(wo_next, t))
        return 0

    lax.fori_loop(0, side, neighbours, 0)

    for b in range(side):
        for copy in kv(2 if b < side // 2 else 3, b, down):
            copy.wait_recv()

    def send(n):
        index, _, a = place.at(0, n)
        columns = pl.ds(pl.multiple_of(place.p * g * d, 128), g * d)
        return _remote(obuf.at[a], o_out.at[:, columns], osend.at[n], orecv.at[n], index)

    def finish(n, _):
        for t in range(side):
            pl.when(n == t + 1)(functools.partial(wo_last, t))
        a = lax.rem(place.p + n, side)
        last = (1 - place.c) * before(2) * side + place.c * (a + before(2))
        lax.fori_loop(0, last, lambda b, _: (unit(a, 3, b), 0)[1], 0)
        for j in range(g):
            mix = mix_s[a * g + j]
            obuf[a, :, j * d : (j + 1) * d] = (mix[:d] * (1 / mix[d : d + 1])).T.astype(low)

        @pl.when(n < side)
        def _():
            send(n).start()

        return 0

    lax.fori_loop(1, side + 1, finish, 0)
    columns = pl.ds(pl.multiple_of(place.p * g * d, 128), g * d)
    keep = pltpu.make_async_copy(obuf.at[place.p], o_out.at[:, columns], olocal)
    keep.start()
    for b in range(side):
        for s in (0, 1, 2 if b < side // 2 else 3):
            for copy in kv(s, b, down):
                copy.wait_send()
    for n in range(1, side):
        send(n).wait()
    keep.wait()
    wo_end()


def solution(mesh):
    side = math.isqrt(mesh.shape["sp"])

    def step(x, gain, wq, wk, wv, wo):
        own, width = x.shape
        heads, kv_heads = wq.shape[1] // HEAD, wk.shape[1] // HEAD
        g = heads // kv_heads
        low = x.dtype
        a = normed(x, gain)
        freq = (THETA ** (-jnp.arange(HEAD // 2, dtype=jnp.float32) / (HEAD // 2)))[None]
        hbm, vmem = pl.BlockSpec(memory_space=pl.ANY), pl.BlockSpec(memory_space=pltpu.VMEM)
        dma = pltpu.SemaphoreType.DMA
        q, k, v = pl.pallas_call(
            functools.partial(_project, side),
            in_specs=[hbm, vmem, hbm, hbm, hbm],
            out_specs=[vmem] * 3,
            out_shape=[
                jax.ShapeDtypeStruct((side * g, own, HEAD), low),
                jax.ShapeDtypeStruct((side, own, HEAD), low),
                jax.ShapeDtypeStruct((side, HEAD, own), low),
            ],
            scratch_shapes=[
                pltpu.VMEM((side, own, width), low),
                pltpu.VMEM((width, (g + 2) * HEAD), low),
                pltpu.VMEM((2 * side, own // 2, HEAD // 2), jnp.float32),
                pltpu.VMEM((2 * side, own // 2, HEAD // 2), jnp.float32),
                dma, dma((3,)), dma((side, 3)), dma((side, 3)), dma((3, side)), dma((3, side)), dma((3, 2)), dma((3, 2)),
            ],
            compiler_params=pltpu.CompilerParams(collective_id=0, has_side_effects=True, vmem_limit_bytes=VMEM),
            cost_estimate=pl.CostEstimate(flops=2 * side * own * width * (g + 2) * HEAD, transcendentals=0, bytes_accessed=side * own * width * 2),
        )(a, freq, wq, wk, wv)
        o, wo = pl.pallas_call(
            functools.partial(_attention, side, HEAD**-0.5),
            in_specs=[vmem, hbm, hbm, hbm],
            out_specs=[hbm, hbm],
            out_shape=[jax.ShapeDtypeStruct((own, heads * HEAD), low), jax.ShapeDtypeStruct((heads * HEAD, width), low)],
            scratch_shapes=[
                pltpu.VMEM((side, side, own, HEAD), low),
                pltpu.VMEM((side, side, HEAD, own), low),
                pltpu.VMEM((side, own, g * HEAD), low),
                pltpu.VMEM((side * g, 1, own), jnp.float32),
                pltpu.VMEM((side * g, HEAD + 8, own), jnp.float32),
                dma((2,)), dma((3, side, 2)), dma((3, side, 2)), dma((side,)), dma((side,)), dma,
                dma((side,)), dma((side,)), dma((3, side)), dma((3, side)), dma((4, side)), dma((4, side)), dma,
            ],
            compiler_params=pltpu.CompilerParams(collective_id=1, has_side_effects=True, vmem_limit_bytes=VMEM),
            cost_estimate=pl.CostEstimate(flops=4 * g * side * own * side * side * own * HEAD // 2, transcendentals=0, bytes_accessed=side * own * width * 2),
        )(q, k, v, wo)
        y = jnp.dot(o, wo, preferred_element_type=jnp.float32)
        return (x.astype(jnp.float32) + y).astype(jnp.bfloat16)

    tokens, whole = P(("dp", "sp"), None), P("sp", None)
    return jax.shard_map(
        step,
        mesh=mesh,
        in_specs=(tokens, P(None), whole, whole, whole, whole),
        out_specs=tokens,
        check_vma=False,
    )
```

```python
import functools
import math

import jax
import jax.numpy as jnp
from jax import lax
from jax.experimental import pallas as pl
from jax.experimental.pallas import tpu as pltpu
from jax.sharding import PartitionSpec as P

HEAD = 256
THETA = 10000
MESH = pl.DeviceIdType.MESH
NEG = -1e30
HIDDEN = 2 * NEG
LOG2E = 1.4426950408889634
VMEM = 60 * 2**20
WO_AT = ((5, 0), (7, 1))


def _dot(a, b, ca, cb):
    return lax.dot_general(a, b, (((ca,), (cb,)), ((), ())), preferred_element_type=jnp.float32)


class Place:
    def __init__(self, side):
        self.side = side
        self.c = lax.rem(lax.axis_index("dp"), 2)
        self.me = lax.axis_index("sp")
        hi, lo = lax.div(self.me, side), lax.rem(self.me, side)
        self.r = (1 - self.c) * hi + self.c * lo
        self.p = (1 - self.c) * lo + self.c * hi

    def at(self, dr, dp):
        r, p = lax.rem(self.r + dr + self.side, self.side), lax.rem(self.p + dp + self.side, self.side)
        return self.block(r, p), r, p

    def block(self, r, p):
        return (1 - self.c) * (r * self.side + p) + self.c * (p * self.side + r)

    def slot(self, n):
        two, odd = lax.div(n, 2), lax.rem(n, 2)
        return lax.rem(self.p + self.side + (1 - odd) * two - odd * (1 - 3 * two), self.side)


def _remote(src, dst, send, recv, index, axis="sp"):
    return pltpu.make_async_remote_copy(src_ref=src, dst_ref=dst, send_sem=send, recv_sem=recv, device_id={axis: index}, device_id_type=MESH)


def _layer(side, scale, x, gain, freq, wq, wk, wv, wo, o_out, wo_out, xbuf, abuf, wbuf, cos_s, sin_s, qbuf, kbuf, vbuf, obuf, top_s, mix_s,
           lsem, w1s, w1r, w2s, w2r, xs, xr, ks, kr, osend, orecv, g1s, g1r, g2s, g2r, ds, dr):
    place = Place(side)
    own, share, d, low = x.shape[0], wq.shape[0], HEAD, x.dtype
    half = own // 2
    g = qbuf.shape[0] // side
    e = scale * LOG2E
    down, up = place.at(1, 0)[0], place.at(-1, 0)[0]
    right, left = place.at(0, 1)[0], place.at(0, -1)[0]
    partner = lax.axis_index("dp") + 1 - 2 * place.c

    load = pltpu.make_async_copy(x, xbuf, lsem.at[0])
    load.start()
    barrier = pltpu.get_barrier_semaphore()
    others = [{"sp": place.at(*t)[0]} for t in [(0, n) for n in range(1, side)] + [(n, 0) for n in range(1, side)]] + [{"dp": partner}]
    for other in others:
        pl.semaphore_signal(barrier, inc=1, device_id=other, device_id_type=MESH)
    pl.semaphore_wait(barrier, len(others))

    parts, off = [], 0
    for w in (wq, wk, wv):
        width = w.shape[1] // side
        parts.append((w, width, off))
        off += width
    rows = lambda index: pl.ds(pl.multiple_of(index * share, 32), share)
    w1 = {}
    for t in range(1, side):
        index, _, to = place.at(0, t)
        for i, (w, width, at) in enumerate(parts):
            columns = pl.ds(pl.multiple_of(to * width, 128), width)
            w1[t, i] = _remote(w.at[:, columns], wbuf.at[rows(place.me), pl.ds(at, width)], w1s.at[t, i], w1r.at[t, i], index)
            w1[t, i].start()
    for i, (w, width, at) in enumerate(parts):
        columns = pl.ds(pl.multiple_of(place.p * width, 128), width)
        w1[0, i] = pltpu.make_async_copy(w.at[:, columns], wbuf.at[rows(place.me), pl.ds(at, width)], lsem.at[i + 1])
        w1[0, i].start()

    load.wait()
    tile = 32

    def norm(n, _):
        here = pl.ds(pl.multiple_of(n * tile, tile), tile)
        wide = xbuf[here, :].astype(jnp.float32)
        by = lax.rsqrt(jnp.mean(wide * wide, -1, keepdims=True) + 1e-6)
        abuf[0, here, :] = (wide * by * gain[...].astype(jnp.float32)).astype(low)
        return 0

    lax.fori_loop(0, own // tile, norm, 0)

    w2 = {}
    def spread(t):
        for i in range(3):
            if t:
                w1[t, i].wait_recv()
            else:
                w1[t, i].wait()
        block = wbuf.at[rows(place.at(0, -t)[0]), :]
        for s, to in ((0, down), (1, up)):
            w2[s, t] = _remote(block, block, w2s.at[s, t], w2r.at[s, t], to)
            w2[s, t].start()

    spread(0)
    part = lambda h: pl.ds(h * half, half)
    states = {}
    for s, to, order in ((0, right, (0, 1)), (1, left, (1, 0))):
        for h in order:
            states[s, h] = _remote(abuf.at[0, part(h), :], abuf.at[s + 1, part(h), :], xs.at[s, h], xr.at[s, h], to)
            states[s, h].start()
    for t in range(1, side):
        spread(t)

    rows_o, wide_o = wo.shape[0], wo.shape[1] // 2
    cols_o = pl.ds(pl.multiple_of(place.c * wide_o, 128), wide_o)

    def piece(to_r, to_p):
        return wo_out.at[pl.ds(pl.multiple_of(place.at(to_r, to_p)[0] * rows_o, rows_o), rows_o), cols_o]

    g1 = {t: _remote(wo.at[:, cols_o], piece(0, 0), g1s.at[t], g1r.at[t], place.at(t, 0)[0]) for t in (1, 3, 2)}
    whole = pltpu.make_async_copy(wo, wo_out.at[pl.ds(pl.multiple_of(place.me * rows_o, rows_o), rows_o), :], lsem.at[4])
    whole.start()

    def along(s, t):
        if s == 2:
            block, to = piece(-t, -1 if t < side // 2 else 1), right if t < side // 2 else left
        else:
            block, to = piece(-t, 0), (right, left)[s]
        if t == 0 and s < 2:
            return _remote(wo.at[:, cols_o], block, g2s.at[s, t], g2r.at[s, t], to)
        return _remote(block, block, g2s.at[s, t], g2r.at[s, t], to)

    def across(n, t):
        block = piece(-t, (0, -1, 1, 2)[n])
        return _remote(block, block, ds.at[n, t], dr.at[n, t], partner, "dp")

    def wo_start():
        for t in range(side):
            if t:
                g1[t].wait_recv()
                across(0, t).start()
            for s in range(2):
                along(s, t).start()

    def wo_next(t):
        for s in range(2):
            along(s, t).wait_recv()
            across(s + 1, t).start()
            if (t < side // 2) == (s == 0):
                along(2, t).start()

    def wo_end():
        for t in range(side):
            along(2, t).wait_recv()
            across(3, t).start()
        for n in range(4):
            for t in range(side):
                if n or t:
                    across(n, t).wait()
        for t in range(side):
            for s in range(3):
                along(s, t).wait_send()
            if t:
                g1[t].wait_send()
        whole.wait()

    def table(n, _):
        first = place.block(place.r, place.slot(lax.div(n, 2))) * own + lax.rem(n, 2) * half
        angle = (lax.broadcasted_iota(jnp.int32, (half, d // 2), 0) + first).astype(jnp.float32) * freq[...]
        cos_s[n] = jnp.cos(angle)
        sin_s[n] = jnp.sin(angle)
        return 0

    lax.fori_loop(0, 2 * side, table, 0)
    top_s[...] = jnp.full(top_s.shape, NEG, jnp.float32)
    mix_s[...] = jnp.zeros(mix_s.shape, jnp.float32)

    def pass_on(s, h, to):
        states[s, h].wait_recv()
        states[2, h] = _remote(abuf.at[s + 1, part(h), :], abuf.at[3, part(h), :], xs.at[2, h], xr.at[2, h], to)
        states[2, h].start()

    for t in range(side):
        for s, to, to_r in ((0, down, -1), (1, up, 1)):
            w2[s, t].wait_recv()
            if (t < side // 2) == (s == 0):
                block = wbuf.at[rows(place.at(to_r, -t)[0]), :]
                w2[2, t] = _remote(block, block, w2s.at[2, t], w2r.at[2, t], to)
                w2[2, t].start()
    for copy in g1.values():
        copy.start()
    pass_on(0, 0, right)
    pass_on(1, 1, left)
    for t in range(side):
        w2[2, t].wait_recv()
    wo_start()

    def kv(s, n):
        b = place.slot(n)
        second = s >= 2 if isinstance(s, int) else 0
        src, slot, i = (s - 1, 3, 2) if second else (0, s + 1, s)
        to = (down, up)[s % 2] if isinstance(s, int) else (1 - s) * down + s * up
        return [_remote(t.at[src, b], t.at[slot, b], ks.at[i, n, m], kr.at[i, n, m], to) for m, t in enumerate((kbuf, vbuf))]

    def turn(t, cos, sin):
        t = t.astype(low)
        lo, hi = t[:, : d // 2].astype(jnp.float32), t[:, d // 2 :].astype(jnp.float32)
        return jnp.concatenate([lo * cos - hi * sin, hi * cos + lo * sin], 1).astype(low)

    ones = jnp.ones((8, own), low)

    def unit(queries, s, keys, masked=False):
        strips = [a * g + j for a in queries for j in range(g)]
        blocks = [kbuf[s, b] for b in keys]
        scores = [[_dot(k, qbuf[i], 1, 1) for k in blocks] for i in strips]
        weights, keeps = [], []
        for i, ts in zip(strips, scores):
            if masked:
                seen = lax.broadcasted_iota(jnp.int32, (own, own), 1) >= lax.broadcasted_iota(jnp.int32, (own, own), 0)
                ts = [jnp.where(seen, t, HIDDEN) for t in ts]
            old = top_s[i]
            top = old
            for t in ts:
                top = jnp.maximum(top, t.max(axis=0, keepdims=True))
            top_s[i] = top
            weights.append([jnp.exp2((t - top) * e).astype(low) for t in ts])
            keeps.append(jnp.exp2((old - top) * e))
        values = [jnp.concatenate([vbuf[s, b], ones], axis=0) for b in keys]
        for i, ws, keep in zip(strips, weights, keeps):
            mix = mix_s[i] * keep
            for v, w in zip(values, ws):
                mix = mix + _dot(v, w, 1, 0)
            mix_s[i] = mix

    def project(n, _):
        for when, (s, h) in ((3, (0, 1)), (4, (1, 0)), (6, (2, 0)), (7, (2, 1))):
            pl.when(n == when)(states[s, h].wait_recv)
        slot, h = lax.div(n, 2), lax.rem(n, 2)
        q = place.slot(slot)
        here = pl.ds(pl.multiple_of(h * half, half), half)
        got = _dot(abuf[slot, here, :], wbuf[...], 1, 0)
        cos, sin = cos_s[n], sin_s[n]
        kbuf[0, q, here, :] = turn(got[:, g * d : (g + 1) * d], cos, sin)
        vbuf[0, q, :, here] = got[:, (g + 1) * d :].astype(low).T
        for j in range(g):
            qbuf[q * g + j, here, :] = turn(got[:, j * d : (j + 1) * d], cos, sin)

        @pl.when(h == 1)
        def _():
            for s in range(2):
                for copy in kv(s, slot):
                    copy.start()
            unit([q], 0, [q], True)

            def other(m, _):
                a = place.slot(m)
                unit([jnp.maximum(a, q)], 0, [jnp.minimum(a, q)])
                return 0

            lax.fori_loop(0, slot, other, 0)

        return 0

    lax.fori_loop(0, 2 * side, project, 0)

    def before(to_r):
        there = lax.rem(place.r + to_r + side, side)
        return lax.div(place.r - there + side - 1, side)

    def first_seeing(to_r, b):
        return (1 - place.c) * (1 - before(to_r)) * side + place.c * (b + 1 - before(to_r))

    def two(first, count, one, both):
        odd = lax.rem(count, 2)
        pl.when(odd == 1)(lambda: one(first))
        lax.fori_loop(0, lax.div(count, 2), lambda i, _: (both(first + odd + 2 * i), 0)[1], 0)

    def block(m, _):
        n, s = lax.div(m, 2), lax.rem(m, 2)
        for copy in kv(s, n):
            copy.wait_recv()
        for side_ in range(2):
            @pl.when((s == side_) & (lax.rem(n, 2) == side_))
            def _():
                for copy in kv(side_ + 2, n):
                    copy.start()

        b = place.slot(n)
        lo = first_seeing(2 * s - 1, b)
        two(lo, side - lo, lambda a: unit([a], s + 1, [b]), lambda a: unit([a, a + 1], s + 1, [b]))
        for at, t in WO_AT:
            pl.when(m == at)(functools.partial(wo_next, t))
        return 0

    lax.fori_loop(0, 2 * side, block, 0)

    for n in range(side):
        for copy in kv(2 + n % 2, n):
            copy.wait_recv()
        if n >= 2:
            wo_next(n)

    columns = pl.ds(pl.multiple_of(place.p * g * d, 128), g * d)

    def send(n):
        index, _, a = place.at(0, n)
        return _remote(obuf.at[a], o_out.at[:, columns], osend.at[n], orecv.at[n], index)

    def finish(n, _):
        a = lax.rem(place.p + n, side)
        last = (1 - place.c) * before(2) * side + place.c * (a + before(2))
        two(0, last, lambda b: unit([a], 3, [b]), lambda b: unit([a], 3, [b, b + 1]))
        for j in range(g):
            mix = mix_s[a * g + j]
            obuf[a, :, j * d : (j + 1) * d] = (mix[:d] * (1 / mix[d : d + 1])).T.astype(low)

        @pl.when(n < side)
        def _():
            send(n).start()

        return 0

    lax.fori_loop(1, side + 1, finish, 0)
    keep = pltpu.make_async_copy(obuf.at[place.p], o_out.at[:, columns], lsem.at[5])
    keep.start()
    for copies in (w1, w2, states):
        for key, copy in copies.items():
            if not (copies is w1 and key[0] == 0):
                copy.wait_send()
    for n in range(side):
        for s in (0, 1, 2 + n % 2):
            for copy in kv(s, n):
                copy.wait_send()
    wo_end()
    for n in range(1, side):
        send(n).wait()
    keep.wait()


def solution(mesh):
    side = math.isqrt(mesh.shape["sp"])

    def step(x, gain, wq, wk, wv, wo):
        own, width = x.shape
        heads, kv_heads = wq.shape[1] // HEAD, wk.shape[1] // HEAD
        g = heads // kv_heads
        low = x.dtype
        freq = (THETA ** (-jnp.arange(HEAD // 2, dtype=jnp.float32) / (HEAD // 2)))[None]
        hbm, vmem = pl.BlockSpec(memory_space=pl.ANY), pl.BlockSpec(memory_space=pltpu.VMEM)
        dma = pltpu.SemaphoreType.DMA
        o, wo = pl.pallas_call(
            functools.partial(_layer, side, HEAD**-0.5),
            in_specs=[hbm, vmem, vmem, hbm, hbm, hbm, hbm],
            out_specs=[hbm, hbm],
            out_shape=[jax.ShapeDtypeStruct((own, heads * HEAD), low), jax.ShapeDtypeStruct((heads * HEAD, width), low)],
            scratch_shapes=[
                pltpu.VMEM((own, width), low),
                pltpu.VMEM((side, own, width), low),
                pltpu.VMEM((width, (g + 2) * HEAD), low),
                pltpu.VMEM((2 * side, own // 2, HEAD // 2), jnp.float32),
                pltpu.VMEM((2 * side, own // 2, HEAD // 2), jnp.float32),
                pltpu.VMEM((side * g, own, HEAD), low),
                pltpu.VMEM((side, side, own, HEAD), low),
                pltpu.VMEM((side, side, HEAD, own), low),
                pltpu.VMEM((side, own, g * HEAD), low),
                pltpu.VMEM((side * g, 1, own), jnp.float32),
                pltpu.VMEM((side * g, HEAD + 8, own), jnp.float32),
                dma((6,)),
                dma((side, 3)), dma((side, 3)), dma((3, side)), dma((3, side)), dma((3, 2)), dma((3, 2)),
                dma((3, side, 2)), dma((3, side, 2)), dma((side,)), dma((side,)),
                dma((side,)), dma((side,)), dma((3, side)), dma((3, side)), dma((4, side)), dma((4, side)),
            ],
            compiler_params=pltpu.CompilerParams(collective_id=0, has_side_effects=True, vmem_limit_bytes=VMEM),
            cost_estimate=pl.CostEstimate(flops=2 * side * own * width * (g + 2) * HEAD, transcendentals=0, bytes_accessed=side * own * width * 2),
        )(x, gain[None], freq, wq, wk, wv, wo)
        y = jnp.dot(o, wo, preferred_element_type=jnp.float32)
        return (x.astype(jnp.float32) + y).astype(jnp.bfloat16)

    tokens, whole = P(("dp", "sp"), None), P("sp", None)
    return jax.shard_map(
        step,
        mesh=mesh,
        in_specs=(tokens, P(None), whole, whole, whole, whole),
        out_specs=tokens,
        check_vma=False,
    )
```

```python
import functools
import math

import jax
import jax.numpy as jnp
import numpy as np
from jax import lax
from jax.experimental import pallas as pl
from jax.experimental.pallas import tpu as pltpu
from jax.sharding import PartitionSpec as P

HEAD = 256
THETA = 10000
MESH = pl.DeviceIdType.MESH
NEG = -1e30
HIDDEN = 2 * NEG
LOG2E = 1.4426950408889634
VMEM = 60 * 2**20
EARLY = 4
WO_AT = (6, 7, 8, 9, 10)


def _dot(a, b, ca, cb):
    return lax.dot_general(a, b, (((ca,), (cb,)), ((), ())), preferred_element_type=jnp.float32)


class Place:
    def __init__(self, side):
        self.side = side
        self.c = lax.rem(lax.axis_index("dp"), 2)
        self.me = lax.axis_index("sp")
        hi, lo = lax.div(self.me, side), lax.rem(self.me, side)
        self.r = (1 - self.c) * hi + self.c * lo
        self.p = (1 - self.c) * lo + self.c * hi

    def at(self, dr, dp):
        r, p = lax.rem(self.r + dr + self.side, self.side), lax.rem(self.p + dp + self.side, self.side)
        return self.block(r, p), r, p

    def block(self, r, p):
        return (1 - self.c) * (r * self.side + p) + self.c * (p * self.side + r)

    def slot(self, n):
        two, odd = lax.div(n, 2), lax.rem(n, 2)
        return lax.rem(self.p + self.side + (1 - odd) * two - odd * (1 - 3 * two), self.side)


def _remote(src, dst, send, recv, index, axis="sp"):
    return pltpu.make_async_remote_copy(src_ref=src, dst_ref=dst, send_sem=send, recv_sem=recv, device_id={axis: index}, device_id_type=MESH)


def _layer(side, scale, x, gain, freq, wq, wk, wv, wo, y_out, wo_out, xbuf, abuf, wbuf, cos_s, sin_s, qbuf, kbuf, vbuf, obuf, home, y_s, top_s, mix_s,
           lsem, w1s, w1r, w2s, w2r, xs, xr, ks, kr, osend, orecv, g1s, g1r, g2s, g2r, ds, dr):
    place = Place(side)
    own, share, d, low = x.shape[0], wq.shape[0], HEAD, x.dtype
    half = own // 2
    g = qbuf.shape[0] // side
    e = scale * LOG2E
    down, up = place.at(1, 0)[0], place.at(-1, 0)[0]
    right, left = place.at(0, 1)[0], place.at(0, -1)[0]
    partner = lax.axis_index("dp") + 1 - 2 * place.c

    load = pltpu.make_async_copy(x, xbuf, lsem.at[0])
    load.start()
    barrier = pltpu.get_barrier_semaphore()
    others = [{"sp": place.at(*t)[0]} for t in [(0, n) for n in range(1, side)] + [(n, 0) for n in range(1, side)]] + [{"dp": partner}]
    for other in others:
        pl.semaphore_signal(barrier, inc=1, device_id=other, device_id_type=MESH)
    pl.semaphore_wait(barrier, len(others))

    parts, off = [], 0
    for w in (wq, wk, wv):
        width = w.shape[1] // side
        parts.append((w, width, off))
        off += width
    rows = lambda index: pl.ds(pl.multiple_of(index * share, 32), share)
    w1 = {}
    for t in range(1, side):
        index, _, to = place.at(0, t)
        for i, (w, width, at) in enumerate(parts):
            columns = pl.ds(pl.multiple_of(to * width, 128), width)
            w1[t, i] = _remote(w.at[:, columns], wbuf.at[rows(place.me), pl.ds(at, width)], w1s.at[t, i], w1r.at[t, i], index)
            w1[t, i].start()
    for i, (w, width, at) in enumerate(parts):
        columns = pl.ds(pl.multiple_of(place.p * width, 128), width)
        w1[0, i] = pltpu.make_async_copy(w.at[:, columns], wbuf.at[rows(place.me), pl.ds(at, width)], lsem.at[i + 1])
        w1[0, i].start()

    load.wait()
    tile = 32

    def norm(n, _):
        here = pl.ds(pl.multiple_of(n * tile, tile), tile)
        wide = xbuf[here, :].astype(jnp.float32)
        by = lax.rsqrt(jnp.mean(wide * wide, -1, keepdims=True) + 1e-6)
        abuf[0, here, :] = (wide * by * gain[...].astype(jnp.float32)[None]).astype(low)
        return 0

    lax.fori_loop(0, own // tile, norm, 0)

    w2 = {}
    def spread(t):
        for i in range(3):
            if t:
                w1[t, i].wait_recv()
            else:
                w1[t, i].wait()
        block = wbuf.at[rows(place.at(0, -t)[0]), :]
        for s, to in ((0, down), (1, up)):
            w2[s, t] = _remote(block, block, w2s.at[s, t], w2r.at[s, t], to)
            w2[s, t].start()

    spread(0)
    part = lambda h: pl.ds(h * half, half)
    states = {}
    for s, to, order in ((0, right, (0, 1)), (1, left, (1, 0))):
        for h in order:
            states[s, h] = _remote(abuf.at[0, part(h), :], abuf.at[s + 1, part(h), :], xs.at[s, h], xr.at[s, h], to)
            states[s, h].start()
    for t in range(1, side):
        spread(t)

    rows_o, wide_o = wo.shape[0], wo.shape[1] // 2
    cols_o = pl.ds(pl.multiple_of(place.c * wide_o, 128), wide_o)

    def piece(to_r, to_p):
        return wo_out.at[pl.ds(pl.multiple_of(place.at(to_r, to_p)[0] * rows_o, rows_o), rows_o), cols_o]

    g1 = {t: _remote(wo.at[:, cols_o], piece(0, 0), g1s.at[t], g1r.at[t], place.at(t, 0)[0]) for t in (1, 3, 2)}
    whole = pltpu.make_async_copy(wo, wo_out.at[pl.ds(pl.multiple_of(place.me * rows_o, rows_o), rows_o), :], lsem.at[4])
    whole.start()

    def along(s, t):
        if s == 2:
            block, to = piece(-t, -1 if t < side // 2 else 1), right if t < side // 2 else left
        else:
            block, to = piece(-t, 0), (right, left)[s]
        if t == 0 and s < 2:
            return _remote(wo.at[:, cols_o], block, g2s.at[s, t], g2r.at[s, t], to)
        return _remote(block, block, g2s.at[s, t], g2r.at[s, t], to)

    def across(n, t):
        block = piece(-t, (0, -1, 1, 2)[n])
        return _remote(block, block, ds.at[n, t], dr.at[n, t], partner, "dp")

    def wo_start():
        for t in range(side):
            if t:
                g1[t].wait_recv()
                across(0, t).start()
            if t < side // 2:
                for s in range(2):
                    along(s, t).start()

    def wo_more():
        for t in range(side // 2, side):
            for s in range(2):
                along(s, t).start()

    def wo_next(t):
        for s in range(2):
            along(s, t).wait_recv()
            across(s + 1, t).start()
            if (t < side // 2) == (s == 0):
                along(2, t).start()

    def wo_end():
        for t in range(side):
            along(2, t).wait_recv()
            across(3, t).start()
        for n in range(4):
            for t in range(side):
                if n or t:
                    across(n, t).wait()
        for t in range(side):
            for s in range(3):
                along(s, t).wait_send()
            if t:
                g1[t].wait_send()
        whole.wait()

    def table(n, _):
        first = place.block(place.r, place.slot(lax.div(n, 2))) * own + lax.rem(n, 2) * half
        angle = (lax.broadcasted_iota(jnp.int32, (half, d // 2), 0) + first).astype(jnp.float32) * freq[...]
        cos_s[n] = jnp.cos(angle)
        sin_s[n] = jnp.sin(angle)
        return 0

    lax.fori_loop(0, 2 * side, table, 0)
    top_s[...] = jnp.full(top_s.shape, NEG, jnp.float32)
    mix_s[...] = jnp.zeros(mix_s.shape, jnp.float32)

    def pass_on(s, h, to):
        states[s, h].wait_recv()
        states[2, h] = _remote(abuf.at[s + 1, part(h), :], abuf.at[3, part(h), :], xs.at[2, h], xr.at[2, h], to)
        states[2, h].start()

    for t in range(side):
        for s, to, to_r in ((0, down, -1), (1, up, 1)):
            w2[s, t].wait_recv()
            if (t < side // 2) == (s == 0):
                block = wbuf.at[rows(place.at(to_r, -t)[0]), :]
                w2[2, t] = _remote(block, block, w2s.at[2, t], w2r.at[2, t], to)
                w2[2, t].start()
    for copy in g1.values():
        copy.start()
    pass_on(0, 0, right)
    pass_on(1, 1, left)
    for t in range(side):
        w2[2, t].wait_recv()

    def kv(s, n):
        b = place.slot(n)
        second = s >= 2 if isinstance(s, int) else 0
        src, slot, i = (s - 1, 3, 2) if second else (0, s + 1, s)
        to = (down, up)[s % 2] if isinstance(s, int) else (1 - s) * down + s * up
        return [_remote(t.at[src, b], t.at[slot, b], ks.at[i, n, m], kr.at[i, n, m], to) for m, t in enumerate((kbuf, vbuf))]

    def turn(t, cos, sin):
        t = t.astype(low)
        lo, hi = t[:, : d // 2].astype(jnp.float32), t[:, d // 2 :].astype(jnp.float32)
        return jnp.concatenate([lo * cos - hi * sin, hi * cos + lo * sin], 1).astype(low)

    ones = jnp.ones((8, own), low)

    def unit(queries, s, keys, masked=False):
        strips = [a * g + j for a in queries for j in range(g)]
        blocks = [kbuf[s, b] for b in keys]
        scores = [[_dot(k, qbuf[i], 1, 1) for k in blocks] for i in strips]
        weights, keeps = [], []
        for i, ts in zip(strips, scores):
            if masked:
                seen = lax.broadcasted_iota(jnp.int32, (own, own), 1) >= lax.broadcasted_iota(jnp.int32, (own, own), 0)
                ts = [jnp.where(seen, t, HIDDEN) for t in ts]
            old = top_s[i]
            top = old
            for t in ts:
                top = jnp.maximum(top, t.max(axis=0, keepdims=True))
            top_s[i] = top
            weights.append([jnp.exp2((t - top) * e).astype(low) for t in ts])
            keeps.append(jnp.exp2((old - top) * e))
        values = [jnp.concatenate([vbuf[s, b], ones], axis=0) for b in keys]
        for i, ws, keep in zip(strips, weights, keeps):
            mix = mix_s[i] * keep
            for v, w in zip(values, ws):
                mix = mix + _dot(v, w, 1, 0)
            mix_s[i] = mix

    def before(to_r):
        there = lax.rem(place.r + to_r + side, side)
        return lax.div(place.r - there + side - 1, side)

    def first_seeing(to_r, b):
        return (1 - place.c) * (1 - before(to_r)) * side + place.c * (b + 1 - before(to_r))

    def two(first, count, one, both):
        odd = lax.rem(count, 2)
        pl.when(odd == 1)(lambda: one(first))
        lax.fori_loop(0, lax.div(count, 2), lambda i, _: (both(first + odd + 2 * i), 0)[1], 0)

    late = place.slot(side - 1)

    def receive(n, s):
        for copy in kv(s, n):
            copy.wait_recv()
        for i in range(2):
            @pl.when((s == i) & (lax.rem(n, 2) == i))
            def _():
                for copy in kv(i + 2, n):
                    copy.start()

    def early(m, _):
        n, s = lax.div(m, 2), lax.rem(m, 2)
        receive(n, s)
        b = place.slot(n)

        def one(a, _):
            pl.when(a != late)(lambda: unit([a], s + 1, [b]))
            return 0

        lax.fori_loop(first_seeing(2 * s - 1, b), side, one, 0)
        return 0

    def project(n, _):
        for when, (s, h) in ((3, (0, 1)), (4, (1, 0)), (6, (2, 0)), (7, (2, 1))):
            pl.when(n == when)(states[s, h].wait_recv)
        slot, h = lax.div(n, 2), lax.rem(n, 2)
        q = place.slot(slot)
        here = pl.ds(pl.multiple_of(h * half, half), half)
        got = _dot(abuf[slot, here, :], wbuf[...], 1, 0)
        cos, sin = cos_s[n], sin_s[n]
        kbuf[0, q, here, :] = turn(got[:, g * d : (g + 1) * d], cos, sin)
        vbuf[0, q, :, here] = got[:, (g + 1) * d :].astype(low).T
        for j in range(g):
            qbuf[q * g + j, here, :] = turn(got[:, j * d : (j + 1) * d], cos, sin)

        @pl.when(h == 1)
        def _():
            for s in range(2):
                for copy in kv(s, slot):
                    copy.start()
            unit([q], 0, [q], True)

            def other(m, _):
                a = place.slot(m)
                unit([jnp.maximum(a, q)], 0, [jnp.minimum(a, q)])
                return 0

            lax.fori_loop(0, slot, other, 0)

        @pl.when(n == 2 * side - 3)
        def _():
            wo_start()
            lax.fori_loop(0, EARLY, early, 0)

        return 0

    lax.fori_loop(0, 2 * side, project, 0)

    def block(m, _):
        far = lax.div(m, 2 * side)
        n, s = (1 - far) * lax.div(m, 2) + far * (m - 2 * side), lax.rem(m, 2)
        slot, to_r = (1 - far) * (s + 1) + far * (side - 1), (1 - far) * (2 * s - 1) + far * 2
        b = place.slot(n)
        lo = first_seeing(to_r, b)

        @pl.when(m < EARLY)
        def _():
            pl.when(late >= lo)(lambda: unit([late], slot, [b]))

        @pl.when(m >= EARLY)
        def _():
            pl.when(far == 0)(lambda: receive(n, s))

            @pl.when(far == 1)
            def _():
                for copy in kv(2, n):
                    copy.wait_recv()

            pl.when(lo == 0)(lambda: unit(list(range(side)), slot, [b]))

            @pl.when(lo > 0)
            def _():
                two(lo, side - lo, lambda a: unit([a], slot, [b]), lambda a: unit([a, a + 1], slot, [b]))

        for at, f in ((WO_AT[0], wo_more), *((at, functools.partial(wo_next, t)) for t, at in enumerate(WO_AT[1:]))):
            pl.when(m == at)(f)
        return 0

    lax.fori_loop(0, 3 * side - 1, block, 0)
    for copy in kv(2, side - 1):
        copy.wait_recv()

    def send(n):
        index, _, a = place.at(0, n)
        return _remote(obuf.at[a], home.at[place.p], osend.at[n], orecv.at[n], index)

    def finish(n, _):
        a = lax.rem(place.p + n, side)
        pl.when(a >= first_seeing(2, late))(lambda: unit([a], 3, [late]))
        for j in range(g):
            mix = mix_s[a * g + j]
            obuf[a, :, j * d : (j + 1) * d] = (mix[:d] * (1 / mix[d : d + 1])).T.astype(low)

        @pl.when(n < side)
        def _():
            send(n).start()

        return 0

    lax.fori_loop(1, side + 1, finish, 0)
    for copies in (w1, w2, states):
        for key, copy in copies.items():
            if not (copies is w1 and key[0] == 0):
                copy.wait_send()
    for n in range(side):
        for s in (0, 1, 2 + n % 2):
            for copy in kv(s, n):
                copy.wait_send()
    wo_end()

    rows_g = wo_out.shape[0] // side

    def fetch(n):
        i = place.at(0, -n)[2]
        return pltpu.make_async_copy(wo_out.at[pl.ds(pl.multiple_of(i * rows_g, rows_g), rows_g), :], abuf.at[i], lsem.at[n])

    for n in range(side):
        fetch(n).start()
    wide = 512

    def add(n, i, o):
        def column(c, _):
            here = pl.ds(pl.multiple_of(c * wide, wide), wide)
            y = _dot(o[i], abuf[i, :, here], 1, 0)
            y = (y_s[:, here] if n else xbuf[:, here].astype(jnp.float32)) + y
            if n < side - 1:
                y_s[:, here] = y
            else:
                y_out[:, here] = y.astype(low)
            return 0

        lax.fori_loop(0, xbuf.shape[1] // wide, column, 0)

    for n in range(side):
        fetch(n).wait()
        if n:
            send(n).wait_recv()
        add(n, place.at(0, -n)[2], home if n else obuf)
    for n in range(1, side):
        send(n).wait_send()


def solution(mesh):
    side = math.isqrt(mesh.shape["sp"])

    def step(x, gain, wq, wk, wv, wo):
        own, width = x.shape
        heads, kv_heads = wq.shape[1] // HEAD, wk.shape[1] // HEAD
        g = heads // kv_heads
        low = x.dtype
        freq = jnp.asarray(np.float32(THETA) ** (-np.arange(HEAD // 2, dtype=np.float32) / np.float32(HEAD // 2)))[None]
        hbm, vmem = pl.BlockSpec(memory_space=pl.ANY), pl.BlockSpec(memory_space=pltpu.VMEM)
        dma = pltpu.SemaphoreType.DMA
        y, _ = pl.pallas_call(
            functools.partial(_layer, side, HEAD**-0.5),
            in_specs=[hbm, vmem, vmem, hbm, hbm, hbm, hbm],
            out_specs=[vmem, hbm],
            out_shape=[jax.ShapeDtypeStruct((own, width), low), jax.ShapeDtypeStruct((heads * HEAD, width), low)],
            scratch_shapes=[
                pltpu.VMEM((own, width), low),
                pltpu.VMEM((side, own, width), low),
                pltpu.VMEM((width, (g + 2) * HEAD), low),
                pltpu.VMEM((2 * side, own // 2, HEAD // 2), jnp.float32),
                pltpu.VMEM((2 * side, own // 2, HEAD // 2), jnp.float32),
                pltpu.VMEM((side * g, own, HEAD), low),
                pltpu.VMEM((side, side, own, HEAD), low),
                pltpu.VMEM((side, side, HEAD, own), low),
                pltpu.VMEM((side, own, g * HEAD), low),
                pltpu.VMEM((side, own, g * HEAD), low),
                pltpu.VMEM((own, width), jnp.float32),
                pltpu.VMEM((side * g, 1, own), jnp.float32),
                pltpu.VMEM((side * g, HEAD + 8, own), jnp.float32),
                dma((6,)),
                dma((side, 3)), dma((side, 3)), dma((3, side)), dma((3, side)), dma((3, 2)), dma((3, 2)),
                dma((3, side, 2)), dma((3, side, 2)), dma((side,)), dma((side,)),
                dma((side,)), dma((side,)), dma((3, side)), dma((3, side)), dma((4, side)), dma((4, side)),
            ],
            compiler_params=pltpu.CompilerParams(collective_id=0, has_side_effects=True, vmem_limit_bytes=VMEM),
            cost_estimate=pl.CostEstimate(flops=2 * side * own * width * (g + 2) * HEAD, transcendentals=0, bytes_accessed=side * own * width * 2),
        )(x, gain, freq, wq, wk, wv, wo)
        return y

    tokens, whole = P(("dp", "sp"), None), P("sp", None)
    return jax.shard_map(
        step,
        mesh=mesh,
        in_specs=(tokens, P(None), whole, whole, whole, whole),
        out_specs=tokens,
        check_vma=False,
    )
```

```python
import functools
import math

import jax
import jax.numpy as jnp
import numpy as np
from jax import lax
from jax.experimental import pallas as pl
from jax.experimental.pallas import tpu as pltpu
from jax.sharding import PartitionSpec as P

HEAD = 256
THETA = 10000
MESH = pl.DeviceIdType.MESH
NEG = -1e30
HIDDEN = 2 * NEG
LOG2E = 1.4426950408889634
VMEM = 60 * 2**20
EARLY = 4
WO_AT = (6, 7, 8, 9, 10)


def _dot(a, b, ca, cb):
    return lax.dot_general(a, b, (((ca,), (cb,)), ((), ())), preferred_element_type=jnp.float32)


class Place:
    def __init__(self, side):
        self.side = side
        self.c = lax.rem(lax.axis_index("dp"), 2)
        self.me = lax.axis_index("sp")
        hi, lo = lax.div(self.me, side), lax.rem(self.me, side)
        self.r = (1 - self.c) * hi + self.c * lo
        self.p = (1 - self.c) * lo + self.c * hi

    def at(self, dr, dp):
        r, p = lax.rem(self.r + dr + self.side, self.side), lax.rem(self.p + dp + self.side, self.side)
        return self.block(r, p), r, p

    def block(self, r, p):
        return (1 - self.c) * (r * self.side + p) + self.c * (p * self.side + r)

    def slot(self, n):
        two, odd = lax.div(n, 2), lax.rem(n, 2)
        return lax.rem(self.p + self.side + (1 - odd) * two - odd * (1 - 3 * two), self.side)


def _remote(src, dst, send, recv, index, axis="sp"):
    return pltpu.make_async_remote_copy(src_ref=src, dst_ref=dst, send_sem=send, recv_sem=recv, device_id={axis: index}, device_id_type=MESH)


def _layer(side, scale, x, gain, freq, wq, wk, wv, wo, y_out, wo_out, xbuf, abuf, wbuf, cos_s, sin_s, qbuf, kbuf, vbuf, obuf, home, y_s, top_s, mix_s,
           lsem, w1s, w1r, w2s, w2r, xs, xr, ks, kr, osend, orecv, g1s, g1r, g2s, g2r, ds, dr):
    place = Place(side)
    own, share, d, low = x.shape[0], wq.shape[0], HEAD, x.dtype
    half = own // 2
    g = qbuf.shape[0] // side
    e = scale * LOG2E
    down, up = place.at(1, 0)[0], place.at(-1, 0)[0]
    right, left = place.at(0, 1)[0], place.at(0, -1)[0]
    partner = lax.axis_index("dp") + 1 - 2 * place.c

    load = pltpu.make_async_copy(x, xbuf, lsem.at[0])
    load.start()
    barrier = pltpu.get_barrier_semaphore()
    others = [{"sp": place.at(*t)[0]} for t in [(0, n) for n in range(1, side)] + [(n, 0) for n in range(1, side)]] + [{"dp": partner}]
    for other in others:
        pl.semaphore_signal(barrier, inc=1, device_id=other, device_id_type=MESH)
    pl.semaphore_wait(barrier, len(others))

    parts, off = [], 0
    for w in (wq, wk, wv):
        width = w.shape[1] // side
        parts.append((w, width, off))
        off += width
    rows = lambda index: pl.ds(pl.multiple_of(index * share, 32), share)
    w1 = {}
    for t in range(1, side):
        index, _, to = place.at(0, t)
        for i, (w, width, at) in enumerate(parts):
            columns = pl.ds(pl.multiple_of(to * width, 128), width)
            w1[t, i] = _remote(w.at[:, columns], wbuf.at[rows(place.me), pl.ds(at, width)], w1s.at[t, i], w1r.at[t, i], index)
            w1[t, i].start()
    for i, (w, width, at) in enumerate(parts):
        columns = pl.ds(pl.multiple_of(place.p * width, 128), width)
        w1[0, i] = pltpu.make_async_copy(w.at[:, columns], wbuf.at[rows(place.me), pl.ds(at, width)], lsem.at[i + 1])
        w1[0, i].start()

    load.wait()
    tile = 32

    def norm(n, _):
        here = pl.ds(pl.multiple_of(n * tile, tile), tile)
        wide = xbuf[here, :].astype(jnp.float32)
        by = lax.rsqrt(jnp.mean(wide * wide, -1, keepdims=True) + 1e-6)
        abuf[0, here, :] = (wide * by * gain[...].astype(jnp.float32)[None]).astype(low)
        return 0

    lax.fori_loop(0, own // tile, norm, 0)

    w2 = {}
    def spread(t):
        for i in range(3):
            if t:
                w1[t, i].wait_recv()
            else:
                w1[t, i].wait()
        block = wbuf.at[rows(place.at(0, -t)[0]), :]
        for s, to in ((0, down), (1, up)):
            w2[s, t] = _remote(block, block, w2s.at[s, t], w2r.at[s, t], to)
            w2[s, t].start()

    spread(0)
    part = lambda h: pl.ds(h * half, half)
    states = {}
    for s, to, order in ((0, right, (0, 1)), (1, left, (1, 0))):
        for h in order:
            states[s, h] = _remote(abuf.at[0, part(h), :], abuf.at[s + 1, part(h), :], xs.at[s, h], xr.at[s, h], to)
            states[s, h].start()
    for t in range(1, side):
        spread(t)

    rows_o, wide_o = wo.shape[0], wo.shape[1] // 2
    cols_o = pl.ds(pl.multiple_of(place.c * wide_o, 128), wide_o)

    def piece(to_r, to_p):
        return wo_out.at[pl.ds(pl.multiple_of(place.at(to_r, to_p)[0] * rows_o, rows_o), rows_o), cols_o]

    g1 = {t: _remote(wo.at[:, cols_o], piece(0, 0), g1s.at[t], g1r.at[t], place.at(t, 0)[0]) for t in (1, 3, 2)}
    whole = pltpu.make_async_copy(wo, wo_out.at[pl.ds(pl.multiple_of(place.me * rows_o, rows_o), rows_o), :], lsem.at[4])
    whole.start()

    def along(s, t):
        if s == 2:
            block, to = piece(-t, -1 if t < side // 2 else 1), right if t < side // 2 else left
        else:
            block, to = piece(-t, 0), (right, left)[s]
        if t == 0 and s < 2:
            return _remote(wo.at[:, cols_o], block, g2s.at[s, t], g2r.at[s, t], to)
        return _remote(block, block, g2s.at[s, t], g2r.at[s, t], to)

    def across(n, t):
        block = piece(-t, (0, -1, 1, 2)[n])
        return _remote(block, block, ds.at[n, t], dr.at[n, t], partner, "dp")

    def wo_start():
        for t in range(side):
            if t:
                g1[t].wait_recv()
                across(0, t).start()
            if t < side // 2:
                for s in range(2):
                    along(s, t).start()

    def wo_more():
        for t in range(side // 2, side):
            for s in range(2):
                along(s, t).start()

    def wo_next(t):
        for s in range(2):
            along(s, t).wait_recv()
            across(s + 1, t).start()
            if (t < side // 2) == (s == 0):
                along(2, t).start()

    def wo_end():
        for t in range(side):
            along(2, t).wait_recv()
            across(3, t).start()
        for n in range(4):
            for t in range(side):
                if n or t:
                    across(n, t).wait()
        for t in range(side):
            for s in range(3):
                along(s, t).wait_send()
            if t:
                g1[t].wait_send()
        whole.wait()

    def table(n, _):
        first = place.block(place.r, place.slot(lax.div(n, 2))) * own + lax.rem(n, 2) * half
        angle = (lax.broadcasted_iota(jnp.int32, (half, d // 2), 0) + first).astype(jnp.float32) * freq[...]
        cos_s[n] = jnp.cos(angle)
        sin_s[n] = jnp.sin(angle)
        return 0

    lax.fori_loop(0, 2 * side, table, 0)
    top_s[...] = jnp.full(top_s.shape, NEG, jnp.float32)
    mix_s[...] = jnp.zeros(mix_s.shape, jnp.float32)

    def pass_on(s, h, to):
        states[s, h].wait_recv()
        states[2, h] = _remote(abuf.at[s + 1, part(h), :], abuf.at[3, part(h), :], xs.at[2, h], xr.at[2, h], to)
        states[2, h].start()

    for t in range(side):
        for s, to, to_r in ((0, down, -1), (1, up, 1)):
            w2[s, t].wait_recv()
            if (t < side // 2) == (s == 0):
                block = wbuf.at[rows(place.at(to_r, -t)[0]), :]
                w2[2, t] = _remote(block, block, w2s.at[2, t], w2r.at[2, t], to)
                w2[2, t].start()
    for copy in g1.values():
        copy.start()
    pass_on(0, 0, right)
    pass_on(1, 1, left)
    for t in range(side):
        w2[2, t].wait_recv()

    def kv(s, n):
        b = place.slot(n)
        second = s >= 2 if isinstance(s, int) else 0
        src, slot, i = (s - 1, 3, 2) if second else (0, s + 1, s)
        to = (down, up)[s % 2] if isinstance(s, int) else (1 - s) * down + s * up
        return [_remote(t.at[src, b], t.at[slot, b], ks.at[i, n, m], kr.at[i, n, m], to) for m, t in enumerate((kbuf, vbuf))]

    def turn(t, cos, sin):
        t = t.astype(low)
        lo, hi = t[:, : d // 2].astype(jnp.float32), t[:, d // 2 :].astype(jnp.float32)
        return jnp.concatenate([lo * cos - hi * sin, hi * cos + lo * sin], 1).astype(low)

    ones = jnp.ones((8, own), low)

    def unit(queries, s, keys, masked=False):
        strips = [a * g + j for a in queries for j in range(g)]
        blocks = [kbuf[s, b] for b in keys]
        scores = [[_dot(k, qbuf[i], 1, 1) for k in blocks] for i in strips]
        weights, keeps = [], []
        for i, ts in zip(strips, scores):
            if masked:
                seen = lax.broadcasted_iota(jnp.int32, (own, own), 1) >= lax.broadcasted_iota(jnp.int32, (own, own), 0)
                ts = [jnp.where(seen, t, HIDDEN) for t in ts]
            old = top_s[i]
            top = old
            for t in ts:
                top = jnp.maximum(top, t.max(axis=0, keepdims=True))
            top_s[i] = top
            weights.append([jnp.exp2((t - top) * e).astype(low) for t in ts])
            keeps.append(jnp.exp2((old - top) * e))
        values = [jnp.concatenate([vbuf[s, b], ones], axis=0) for b in keys]
        for i, ws, keep in zip(strips, weights, keeps):
            mix = mix_s[i] * keep
            for v, w in zip(values, ws):
                mix = mix + _dot(v, w, 1, 0)
            mix_s[i] = mix

    def before(to_r):
        there = lax.rem(place.r + to_r + side, side)
        return lax.div(place.r - there + side - 1, side)

    def first_seeing(to_r, b):
        return (1 - place.c) * (1 - before(to_r)) * side + place.c * (b + 1 - before(to_r))

    def two(first, count, one, both):
        odd = lax.rem(count, 2)
        pl.when(odd == 1)(lambda: one(first))
        lax.fori_loop(0, lax.div(count, 2), lambda i, _: (both(first + odd + 2 * i), 0)[1], 0)

    late = place.slot(side - 1)

    def receive(n, s):
        for copy in kv(s, n):
            copy.wait_recv()
        for i in range(2):
            @pl.when((s == i) & (lax.rem(n, 2) == i))
            def _():
                for copy in kv(i + 2, n):
                    copy.start()

    def early(m, _):
        n, s = lax.div(m, 2), lax.rem(m, 2)
        receive(n, s)
        b = place.slot(n)

        def one(a, _):
            pl.when(a != late)(lambda: unit([a], s + 1, [b]))
            return 0

        lax.fori_loop(first_seeing(2 * s - 1, b), side, one, 0)
        return 0

    def project(n, _):
        for when, (s, h) in ((3, (0, 1)), (4, (1, 0)), (6, (2, 0)), (7, (2, 1))):
            pl.when(n == when)(states[s, h].wait_recv)
        slot, h = lax.div(n, 2), lax.rem(n, 2)
        q = place.slot(slot)
        here = pl.ds(pl.multiple_of(h * half, half), half)
        got = _dot(abuf[slot, here, :], wbuf[...], 1, 0)
        cos, sin = cos_s[n], sin_s[n]
        kbuf[0, q, here, :] = turn(got[:, g * d : (g + 1) * d], cos, sin)
        vbuf[0, q, :, here] = got[:, (g + 1) * d :].astype(low).T
        for j in range(g):
            qbuf[q * g + j, here, :] = turn(got[:, j * d : (j + 1) * d], cos, sin)

        @pl.when(h == 1)
        def _():
            for s in range(2):
                for copy in kv(s, slot):
                    copy.start()
            unit([q], 0, [q], True)

            def other(m, _):
                a = place.slot(m)
                unit([jnp.maximum(a, q)], 0, [jnp.minimum(a, q)])
                return 0

            lax.fori_loop(0, slot, other, 0)

        @pl.when(n == 2 * side - 3)
        def _():
            lax.fori_loop(0, EARLY, early, 0)

        return 0

    lax.fori_loop(0, 2 * side, project, 0)

    def block(m, _):
        far = lax.div(m, 2 * side)
        n, s = (1 - far) * lax.div(m, 2) + far * (m - 2 * side), lax.rem(m, 2)
        slot, to_r = (1 - far) * (s + 1) + far * (side - 1), (1 - far) * (2 * s - 1) + far * 2
        b = place.slot(n)
        lo = first_seeing(to_r, b)

        @pl.when(m < EARLY)
        def _():
            pl.when(late >= lo)(lambda: unit([late], slot, [b]))

        @pl.when(m >= EARLY)
        def _():
            pl.when(far == 0)(lambda: receive(n, s))

            @pl.when(far == 1)
            def _():
                for copy in kv(2, n):
                    copy.wait_recv()

            pl.when(lo == 0)(lambda: unit(list(range(side)), slot, [b]))

            @pl.when(lo > 0)
            def _():
                two(lo, side - lo, lambda a: unit([a], slot, [b]), lambda a: unit([a, a + 1], slot, [b]))

        for at, f in ((0, wo_start), (WO_AT[0], wo_more), *((at, functools.partial(wo_next, t)) for t, at in enumerate(WO_AT[1:]))):
            pl.when(m == at)(f)
        return 0

    lax.fori_loop(0, 3 * side - 1, block, 0)
    for copy in kv(2, side - 1):
        copy.wait_recv()

    def send(n):
        index, _, a = place.at(0, n)
        return _remote(obuf.at[a], home.at[place.p], osend.at[n], orecv.at[n], index)

    def finish(n, _):
        a = lax.rem(place.p + n, side)
        pl.when(a >= first_seeing(2, late))(lambda: unit([a], 3, [late]))
        for j in range(g):
            mix = mix_s[a * g + j]
            obuf[a, :, j * d : (j + 1) * d] = (mix[:d] * (1 / mix[d : d + 1])).T.astype(low)

        @pl.when(n < side)
        def _():
            send(n).start()

        return 0

    lax.fori_loop(1, side + 1, finish, 0)
    for copies in (w1, w2, states):
        for key, copy in copies.items():
            if not (copies is w1 and key[0] == 0):
                copy.wait_send()
    for n in range(side):
        for s in (0, 1, 2 + n % 2):
            for copy in kv(s, n):
                copy.wait_send()
    wo_end()

    rows_g = wo_out.shape[0] // side

    def fetch(n):
        i = place.at(0, -n)[2]
        return pltpu.make_async_copy(wo_out.at[pl.ds(pl.multiple_of(i * rows_g, rows_g), rows_g), :], abuf.at[i], lsem.at[n])

    for n in range(side):
        fetch(n).start()
    wide = 512

    def add(n, i, o):
        def column(c, _):
            here = pl.ds(pl.multiple_of(c * wide, wide), wide)
            y = _dot(o[i], abuf[i, :, here], 1, 0)
            y = (y_s[:, here] if n else xbuf[:, here].astype(jnp.float32)) + y
            if n < side - 1:
                y_s[:, here] = y
            else:
                y_out[:, here] = y.astype(low)
            return 0

        lax.fori_loop(0, xbuf.shape[1] // wide, column, 0)

    for n in range(side):
        fetch(n).wait()
        if n:
            send(n).wait_recv()
        add(n, place.at(0, -n)[2], home if n else obuf)
    for n in range(1, side):
        send(n).wait_send()


def solution(mesh):
    side = math.isqrt(mesh.shape["sp"])

    def step(x, gain, wq, wk, wv, wo):
        own, width = x.shape
        heads, kv_heads = wq.shape[1] // HEAD, wk.shape[1] // HEAD
        g = heads // kv_heads
        low = x.dtype
        freq = jnp.asarray(np.float32(THETA) ** (-np.arange(HEAD // 2, dtype=np.float32) / np.float32(HEAD // 2)))[None]
        hbm, vmem = pl.BlockSpec(memory_space=pl.ANY), pl.BlockSpec(memory_space=pltpu.VMEM)
        dma = pltpu.SemaphoreType.DMA
        y, _ = pl.pallas_call(
            functools.partial(_layer, side, HEAD**-0.5),
            in_specs=[hbm, vmem, vmem, hbm, hbm, hbm, hbm],
            out_specs=[vmem, hbm],
            out_shape=[jax.ShapeDtypeStruct((own, width), low), jax.ShapeDtypeStruct((heads * HEAD, width), low)],
            scratch_shapes=[
                pltpu.VMEM((own, width), low),
                pltpu.VMEM((side, own, width), low),
                pltpu.VMEM((width, (g + 2) * HEAD), low),
                pltpu.VMEM((2 * side, own // 2, HEAD // 2), jnp.float32),
                pltpu.VMEM((2 * side, own // 2, HEAD // 2), jnp.float32),
                pltpu.VMEM((side * g, own, HEAD), low),
                pltpu.VMEM((side, side, own, HEAD), low),
                pltpu.VMEM((side, side, HEAD, own), low),
                pltpu.VMEM((side, own, g * HEAD), low),
                pltpu.VMEM((side, own, g * HEAD), low),
                pltpu.VMEM((own, width), jnp.float32),
                pltpu.VMEM((side * g, 1, own), jnp.float32),
                pltpu.VMEM((side * g, HEAD + 8, own), jnp.float32),
                dma((6,)),
                dma((side, 3)), dma((side, 3)), dma((3, side)), dma((3, side)), dma((3, 2)), dma((3, 2)),
                dma((3, side, 2)), dma((3, side, 2)), dma((side,)), dma((side,)),
                dma((side,)), dma((side,)), dma((3, side)), dma((3, side)), dma((4, side)), dma((4, side)),
            ],
            compiler_params=pltpu.CompilerParams(collective_id=0, has_side_effects=True, vmem_limit_bytes=VMEM),
            cost_estimate=pl.CostEstimate(flops=2 * side * own * width * (g + 2) * HEAD, transcendentals=0, bytes_accessed=side * own * width * 2),
        )(x, gain, freq, wq, wk, wv, wo)
        return y

    tokens, whole = P(("dp", "sp"), None), P("sp", None)
    return jax.shard_map(
        step,
        mesh=mesh,
        in_specs=(tokens, P(None), whole, whole, whole, whole),
        out_specs=tokens,
        check_vma=False,
    )
```
